8 devices in a mesh: dp: 1 (over z), col: 2 (over y), row: 4 (over x, core).
Axes of the slice: x: 2, y: 2, z: 1, core: 2. Of those that a mesh axis runs over, the one named last changes fastest.
Arguments:
- a_mat: bfloat16 [8192, 8192], P(('dp', 'row'), 'col')
- b_mat: bfloat16 [8192, 28672], P('row', 'col')
Outputs:
- output: bfloat16 [8192, 28672], P(('dp', 'row'), 'col')
All inputs are finite; a program needn't handle non-finite values.
Results may differ from the reference program's by a relative error of at most 0.001.
Values are sent between devices in bfloat16 or wider.
A program may use at most 1 GiB of HBM per device.

```python
import jax
import jax.numpy as jnp
from jax import lax

M_ROWS = 8192
K_INNER = 8192
N_COLS = 28672
ROW_BLOCK = 256


def setup_inputs(seed: int = 0, part: int = 0) -> dict:
    base_key = jax.random.key(seed)
    key_a = jax.random.fold_in(jax.random.fold_in(base_key, 1), part)
    key_b = jax.random.fold_in(base_key, 2)
    a_mat = jax.random.normal(key_a, (M_ROWS, K_INNER), jnp.float32).astype(jnp.bfloat16)
    b_mat = (jax.random.normal(key_b, (K_INNER, N_COLS), jnp.float32) * (K_INNER ** -0.5)).astype(jnp.bfloat16)
    return {"a_mat": a_mat, "b_mat": b_mat}


def reference(a_mat, b_mat):
    row_tiles = a_mat.reshape(M_ROWS // ROW_BLOCK, ROW_BLOCK, K_INNER)

    def tile_product(a_tile):
        return jnp.dot(a_tile, b_mat, preferred_element_type=jnp.float32).astype(jnp.bfloat16)

    out_tiles = lax.map(tile_product, row_tiles)
    return out_tiles.reshape(M_ROWS, N_COLS)
```

```python
import jax
import jax.numpy as jnp
from jax import lax
from jax.experimental import pallas as pl
from jax.experimental.pallas import tpu as pltpu
from jax.sharding import PartitionSpec as P


UNIT = 256
PIECES = (2, 8, 10, 10, 10, 8, 4, 2, 1, 1)


def product_body(core_ref, a0, a1, a2, a3, b0, b1, b2, b3, *rest):
    c_ref = rest[-1]
    total = jnp.dot(a0[...], b0[...], preferred_element_type=jnp.float32)
    total += jnp.dot(a1[...], b1[...], preferred_element_type=jnp.float32)
    total += jnp.dot(a2[...], b2[...], preferred_element_type=jnp.float32)
    total += jnp.dot(a3[...], b3[...], preferred_element_type=jnp.float32)
    c_ref[...] = total.astype(c_ref.dtype)


def product(core, a_near, a_far, b_own, b_pair, x_own, x_pair, c_prev, start, tm=512):
    rows = a_near.shape[0]
    depth, columns = b_own.shape
    width = x_own.shape[1]
    tn = 512 if width % 512 == 0 and start % 512 == 0 else 256
    first = start // tn
    a_mine = pl.BlockSpec((tm, depth), lambda n, m, core: (m, core[0]))
    a_other = pl.BlockSpec((tm, depth), lambda n, m, core: (m, 1 - core[0]))
    b_whole = pl.BlockSpec((depth, tn), lambda n, m, core: (0, first + n))
    b_piece = pl.BlockSpec((depth, tn), lambda n, m, core: (0, n))
    in_specs = [a_mine, a_other, a_mine, a_other, b_whole, b_whole, b_piece, b_piece]
    args = [a_near, a_near, a_far, a_far, b_own, b_pair, x_own, x_pair]
    aliases = {}
    if c_prev is not None:
        in_specs.append(pl.BlockSpec(memory_space=pl.ANY))
        aliases = {1 + len(args): 0}
        args.append(c_prev)
    return pl.pallas_call(
        product_body,
        grid_spec=pltpu.PrefetchScalarGridSpec(
            num_scalar_prefetch=1,
            grid=(width // tn, rows // tm),
            in_specs=in_specs,
            out_specs=pl.BlockSpec((tm, tn), lambda n, m, core: (m, first + n)),
        ),
        out_shape=jax.ShapeDtypeStruct((rows, columns), jnp.bfloat16),
        input_output_aliases=aliases,
        cost_estimate=pl.CostEstimate(
            flops=2 * rows * 4 * depth * width,
            bytes_accessed=2 * (rows * 4 * depth * (width // tn) + 4 * depth * width + rows * width),
            transcendentals=0,
        ),
        compiler_params=pltpu.CompilerParams(vmem_limit_bytes=62 * 1024 * 1024),
    )(core, *args)


def solution(mesh):
    across = [(0, 2), (2, 0), (1, 3), (3, 1)]
    beside = [(0, 1), (1, 0), (2, 3), (3, 2)]
    pieces = []
    start = 0
    for n in PIECES:
        pieces.append((start, n * UNIT))
        start += n * UNIT

    def local_product(a_blk, b_blk):
        row_id = lax.axis_index("row")
        core = lax.rem(row_id, 2).astype(jnp.int32).reshape(1)
        aligned = lax.div(row_id, 2) == lax.axis_index("col")
        x_own = []
        for s, w in pieces:
            piece = lax.slice_in_dim(b_blk, s, s + w, axis=1)
            x_own.append(lax.ppermute(piece, "row", across))
        a_recv = lax.ppermute(a_blk, "col", [(0, 1), (1, 0)])
        b_pair = lax.ppermute(b_blk, "row", beside)
        a_near = jnp.where(aligned, a_blk, a_recv)
        a_far = jnp.where(aligned, a_recv, a_blk)
        c = None
        for j, (s, w) in enumerate(pieces):
            x = x_own[j]
            if j:
                x, c = lax.optimization_barrier((x, c))
            x_pair = lax.ppermute(x, "row", beside)
            c = product(core, a_near, a_far, b_blk, b_pair, x, x_pair, c, s)
        return c

    return jax.shard_map(
        local_product,
        mesh=mesh,
        in_specs=(P(("dp", "row"), "col"), P("row", "col")),
        out_specs=P(("dp", "row"), "col"),
        check_vma=False,
    )
```

```python
import jax
import jax.numpy as jnp
from jax import lax
from jax.experimental import pallas as pl
from jax.experimental.pallas import tpu as pltpu
from jax.sharding import PartitionSpec as P


PIECES = (
    (128, 0, 1), (896, 0, 1), (2560, 0, 1), (2560, 0, 1), (2560, 0, 1), (2048, 0, 1), (1536, 0, 1),
    (1024, 0, 1), (512, 0, 1), (256, 0, 1), (256, 0, 2), (256, 1, 2),
)
TAIL = 7
NEAR_AFTER = 4
MIB = 1024 * 1024


def matmul_cost(rows, depth, width, tiles):
    return pl.CostEstimate(
        flops=2 * rows * depth * width,
        bytes_accessed=2 * (rows * depth * tiles + depth * width + rows * width),
        transcendentals=0,
    )


def whole_body(core_ref, a0, a1, a2, a3, b0, b1, b2, b3, *rest):
    c_ref = rest[-1]
    total = jnp.dot(a0[...], b0[...], preferred_element_type=jnp.float32)
    total += jnp.dot(a1[...], b1[...], preferred_element_type=jnp.float32)
    total += jnp.dot(a2[...], b2[...], preferred_element_type=jnp.float32)
    total += jnp.dot(a3[...], b3[...], preferred_element_type=jnp.float32)
    c_ref[...] = total.astype(c_ref.dtype)


def tile_of(start, width):
    for tn in (512, 256, 128):
        if start % tn == 0 and width % tn == 0:
            return tn


def whole_product(core, a_near, a_far, b_own, b_pair, x_own, x_pair, c_prev, start, tm=512):
    rows = a_near.shape[0]
    depth, columns = b_own.shape
    width = x_own.shape[1]
    tn = tile_of(start, width)
    first = start // tn
    a_mine = pl.BlockSpec((tm, depth), lambda n, m, core: (m, core[0]))
    a_other = pl.BlockSpec((tm, depth), lambda n, m, core: (m, 1 - core[0]))
    b_whole = pl.BlockSpec((depth, tn), lambda n, m, core: (0, first + n))
    b_piece = pl.BlockSpec((depth, tn), lambda n, m, core: (0, n))
    in_specs = [a_mine, a_other, a_mine, a_other, b_whole, b_whole, b_piece, b_piece]
    args = [a_near, a_near, a_far, a_far, b_own, b_pair, x_own, x_pair]
    aliases = {}
    if c_prev is not None:
        in_specs.append(pl.BlockSpec(memory_space=pl.ANY))
        aliases = {1 + len(args): 0}
        args.append(c_prev)
    return pl.pallas_call(
        whole_body,
        grid_spec=pltpu.PrefetchScalarGridSpec(
            num_scalar_prefetch=1,
            grid=(width // tn, rows // tm),
            in_specs=in_specs,
            out_specs=pl.BlockSpec((tm, tn), lambda n, m, core: (m, first + n)),
        ),
        out_shape=jax.ShapeDtypeStruct((rows, columns), jnp.bfloat16),
        input_output_aliases=aliases,
        cost_estimate=matmul_cost(rows, 4 * depth, width, width // tn),
        compiler_params=pltpu.CompilerParams(vmem_limit_bytes=62 * MIB),
    )(core, *args)


def near_body(core_ref, a0, a1, b0, b1, s_ref):
    s_ref[...] = jnp.dot(a0[...], b0[...], preferred_element_type=jnp.float32)
    s_ref[...] += jnp.dot(a1[...], b1[...], preferred_element_type=jnp.float32)


def near_sums(core, a_near, b_own, b_pair, start, tm=512, tn=512):
    rows = a_near.shape[0]
    depth, columns = b_own.shape
    width = columns - start
    first = start // tn
    b_whole = pl.BlockSpec((depth, tn), lambda n, m, core: (0, first + n))
    return pl.pallas_call(
        near_body,
        grid_spec=pltpu.PrefetchScalarGridSpec(
            num_scalar_prefetch=1,
            grid=(width // tn, rows // tm),
            in_specs=[
                pl.BlockSpec((tm, depth), lambda n, m, core: (m, core[0])),
                pl.BlockSpec((tm, depth), lambda n, m, core: (m, 1 - core[0])),
                b_whole,
                b_whole,
            ],
            out_specs=pl.BlockSpec((tm, tn), lambda n, m, core: (m, n)),
        ),
        out_shape=jax.ShapeDtypeStruct((rows, width), jnp.float32),
        cost_estimate=matmul_cost(rows, 2 * depth, width, width // tn),
        compiler_params=pltpu.CompilerParams(vmem_limit_bytes=62 * MIB),
        name="near",
    )(core, a_near, a_near, b_own, b_pair)


def far_body(core_ref, a0, a1, b0, b1, s_ref, *rest):
    out_ref = rest[-1]
    total = s_ref[...]
    total += jnp.dot(a0[...], b0[...], preferred_element_type=jnp.float32)
    total += jnp.dot(a1[...], b1[...], preferred_element_type=jnp.float32)
    out_ref[...] = total.astype(out_ref.dtype)


def far_product(core, a_far, x_own, x_pair, sums, sums_start, part, parts, c_prev, start, tm=256):
    rows = a_far.shape[0]
    depth, width = x_own.shape
    tn = tile_of(start, width)
    first = start // tn
    sums_first = sums_start // tn
    a_mine = pl.BlockSpec((tm, depth), lambda n, m, core: (m, core[0] * parts + part))
    a_other = pl.BlockSpec((tm, depth), lambda n, m, core: (m, (1 - core[0]) * parts + part))
    b_piece = pl.BlockSpec((depth, tn), lambda n, m, core: (0, n))
    in_specs = [
        a_mine, a_other, b_piece, b_piece, pl.BlockSpec((tm, tn), lambda n, m, core: (m, sums_first + n)),
    ]
    args = [a_far, a_far, x_own, x_pair, sums]
    if c_prev is None:
        out_specs = pl.BlockSpec((tm, tn), lambda n, m, core: (m, n))
        out_shape = jax.ShapeDtypeStruct((rows, width), jnp.float32)
        aliases = {}
    else:
        in_specs.append(pl.BlockSpec(memory_space=pl.ANY))
        aliases = {1 + len(args): 0}
        args.append(c_prev)
        out_specs = pl.BlockSpec((tm, tn), lambda n, m, core: (m, first + n))
        out_shape = jax.ShapeDtypeStruct(c_prev.shape, c_prev.dtype)
    return pl.pallas_call(
        far_body,
        grid_spec=pltpu.PrefetchScalarGridSpec(
            num_scalar_prefetch=1,
            grid=(width // tn, rows // tm),
            in_specs=in_specs,
            out_specs=out_specs,
        ),
        out_shape=out_shape,
        input_output_aliases=aliases,
        cost_estimate=matmul_cost(rows, 2 * depth, width, width // tn),
        compiler_params=pltpu.CompilerParams(vmem_limit_bytes=FAR_VMEM * MIB),
    )(core, *args)


FAR_VMEM = 28


def solution(mesh):
    across = [(0, 2), (2, 0), (1, 3), (3, 1)]
    beside = [(0, 1), (1, 0), (2, 3), (3, 2)]

    def local_product(a_blk, b_blk):
        depth = b_blk.shape[0]
        row_id = lax.axis_index("row")
        core = lax.rem(row_id, 2).astype(jnp.int32).reshape(1)
        aligned = lax.div(row_id, 2) == lax.axis_index("col")
        starts = []
        x_own = []
        begin = 0
        for width, part, parts in PIECES:
            starts.append(begin)
            rows = depth // parts
            piece = lax.slice(b_blk, (part * rows, begin), ((part + 1) * rows, begin + width))
            x_own.append(lax.ppermute(piece, "row", across))
            if part == parts - 1:
                begin += width
        a_recv = lax.ppermute(a_blk, "col", [(0, 1), (1, 0)])
        b_pair = lax.ppermute(b_blk, "row", beside)
        a_near = jnp.where(aligned, a_blk, a_recv)
        a_far = jnp.where(aligned, a_recv, a_blk)
        c = None
        half = None
        for j, (width, part, parts) in enumerate(PIECES):
            x = x_own[j]
            if half is not None:
                x, half = lax.optimization_barrier((x, half))
            elif j:
                x, c = lax.optimization_barrier((x, c))
            x_pair = lax.ppermute(x, "row", beside)
            if j < TAIL:
                c = whole_product(core, a_near, a_far, b_blk, b_pair, x, x_pair, c, starts[j])
            elif part < parts - 1:
                half = far_product(core, a_far, x, x_pair, sums, starts[j] - starts[TAIL], part, parts, None, starts[j])
            elif half is not None:
                c = far_product(core, a_far, x, x_pair, half, 0, part, parts, c, starts[j])
                half = None
            else:
                c = far_product(core, a_far, x, x_pair, sums, starts[j] - starts[TAIL], part, parts, c, starts[j])
            if j == NEAR_AFTER:
                core, c = lax.optimization_barrier((core, c))
                sums = near_sums(core, a_near, b_blk, b_pair, starts[TAIL])
        return c

    return jax.shard_map(
        local_product,
        mesh=mesh,
        in_specs=(P(("dp", "row"), "col"), P("row", "col")),
        out_specs=P(("dp", "row"), "col"),
        check_vma=False,
    )
```

```python
import functools

import jax
import jax.numpy as jnp
from jax import lax
from jax.experimental import pallas as pl
from jax.experimental.pallas import tpu as pltpu
from jax.sharding import PartitionSpec as P


PIECES = (
    (128, 0, 1), (896, 0, 1), (2560, 0, 1), (2560, 0, 1), (2560, 0, 1), (2048, 0, 1), (1536, 0, 1),
    (1024, 0, 1), (512, 0, 1), (256, 0, 1), (256, 0, 2), (256, 1, 2),
)
TAIL = 7
NEAR_AFTER = 4
MIB = 1024 * 1024


def matmul_cost(rows, depth, width, tiles):
    return pl.CostEstimate(
        flops=2 * rows * depth * width,
        bytes_accessed=2 * (rows * depth * tiles + depth * width + rows * width),
        transcendentals=0,
    )


def whole_body(core_ref, a0, a1, a2, a3, b0, b1, b2, b3, *rest):
    c_ref = rest[-1]
    total = jnp.dot(a0[...], b0[...], preferred_element_type=jnp.float32)
    total += jnp.dot(a1[...], b1[...], preferred_element_type=jnp.float32)
    total += jnp.dot(a2[...], b2[...], preferred_element_type=jnp.float32)
    total += jnp.dot(a3[...], b3[...], preferred_element_type=jnp.float32)
    c_ref[...] = total.astype(c_ref.dtype)


def tile_of(start, width):
    for tn in (512, 256, 128):
        if start % tn == 0 and width % tn == 0:
            return tn


def whole_product(core, a_near, a_far, b_own, b_pair, x_own, x_pair, c_prev, start, tm=512):
    rows = a_near.shape[0]
    depth, columns = b_own.shape
    width = x_own.shape[1]
    tn = tile_of(start, width)
    first = start // tn
    a_mine = pl.BlockSpec((tm, depth), lambda n, m, core: (m, core[0]))
    a_other = pl.BlockSpec((tm, depth), lambda n, m, core: (m, 1 - core[0]))
    b_whole = pl.BlockSpec((depth, tn), lambda n, m, core: (0, first + n))
    b_piece = pl.BlockSpec((depth, tn), lambda n, m, core: (0, n))
    in_specs = [a_mine, a_other, a_mine, a_other, b_whole, b_whole, b_piece, b_piece]
    args = [a_near, a_near, a_far, a_far, b_own, b_pair, x_own, x_pair]
    aliases = {}
    if c_prev is not None:
        in_specs.append(pl.BlockSpec(memory_space=pl.ANY))
        aliases = {1 + len(args): 0}
        args.append(c_prev)
    return pl.pallas_call(
        whole_body,
        grid_spec=pltpu.PrefetchScalarGridSpec(
            num_scalar_prefetch=1,
            grid=(width // tn, rows // tm),
            in_specs=in_specs,
            out_specs=pl.BlockSpec((tm, tn), lambda n, m, core: (m, first + n)),
        ),
        out_shape=jax.ShapeDtypeStruct((rows, columns), jnp.bfloat16),
        input_output_aliases=aliases,
        cost_estimate=matmul_cost(rows, 4 * depth, width, width // tn),
        compiler_params=pltpu.CompilerParams(vmem_limit_bytes=62 * MIB),
    )(core, *args)


def near_body(core_ref, a0, a1, b0, b1, s_ref):
    s_ref[...] = jnp.dot(a0[...], b0[...], preferred_element_type=jnp.float32)
    s_ref[...] += jnp.dot(a1[...], b1[...], preferred_element_type=jnp.float32)


def near_sums(core, a_near, b_own, b_pair, start, tm=512, tn=512):
    rows = a_near.shape[0]
    depth, columns = b_own.shape
    width = columns - start
    first = start // tn
    b_whole = pl.BlockSpec((depth, tn), lambda n, m, core: (0, first + n))
    return pl.pallas_call(
        near_body,
        grid_spec=pltpu.PrefetchScalarGridSpec(
            num_scalar_prefetch=1,
            grid=(width // tn, rows // tm),
            in_specs=[
                pl.BlockSpec((tm, depth), lambda n, m, core: (m, core[0])),
                pl.BlockSpec((tm, depth), lambda n, m, core: (m, 1 - core[0])),
                b_whole,
                b_whole,
            ],
            out_specs=pl.BlockSpec((tm, tn), lambda n, m, core: (m, n)),
        ),
        out_shape=jax.ShapeDtypeStruct((rows, width), jnp.float32),
        cost_estimate=matmul_cost(rows, 2 * depth, width, width // tn),
        compiler_params=pltpu.CompilerParams(vmem_limit_bytes=62 * MIB),
        name="near",
    )(core, a_near, a_near, b_own, b_pair)


def far_body(count, core_ref, *refs):
    a_refs, b_refs = refs[:count], refs[count : 2 * count]
    s_ref, out_ref = refs[2 * count], refs[-1]
    total = s_ref[...]
    for a_ref, b_ref in zip(a_refs, b_refs):
        total += jnp.dot(a_ref[...], b_ref[...], preferred_element_type=jnp.float32)
    out_ref[...] = total.astype(out_ref.dtype)


def far_product(core, a_far, x_own, x_pair, sums, sums_start, part, parts, c_prev, start, tm=1024):
    rows = a_far.shape[0]
    depth, width = (x_pair if x_own is None else x_own).shape
    tn = min(256, tile_of(start, width))
    first = start // tn
    sums_first = sums_start // tn
    a_mine = pl.BlockSpec((tm, depth), lambda n, m, core: (m, core[0] * parts + part))
    a_other = pl.BlockSpec((tm, depth), lambda n, m, core: (m, (1 - core[0]) * parts + part))
    b_piece = pl.BlockSpec((depth, tn), lambda n, m, core: (0, n))
    pairs = [(a, x) for a, x in ((a_mine, x_own), (a_other, x_pair)) if x is not None]
    in_specs = [a for a, _ in pairs] + [b_piece] * len(pairs)
    in_specs.append(pl.BlockSpec((tm, tn), lambda n, m, core: (m, sums_first + n)))
    args = [a_far] * len(pairs) + [x for _, x in pairs] + [sums]
    if c_prev is None:
        out_specs = pl.BlockSpec((tm, tn), lambda n, m, core: (m, n))
        out_shape = jax.ShapeDtypeStruct((rows, width), jnp.float32)
        aliases = {len(args): 0} if sums.shape == (rows, width) else {}
    else:
        in_specs.append(pl.BlockSpec(memory_space=pl.ANY))
        aliases = {1 + len(args): 0}
        args.append(c_prev)
        out_specs = pl.BlockSpec((tm, tn), lambda n, m, core: (m, first + n))
        out_shape = jax.ShapeDtypeStruct(c_prev.shape, c_prev.dtype)
    return pl.pallas_call(
        functools.partial(far_body, len(pairs)),
        grid_spec=pltpu.PrefetchScalarGridSpec(
            num_scalar_prefetch=1,
            grid=(width // tn, rows // tm),
            in_specs=in_specs,
            out_specs=out_specs,
        ),
        out_shape=out_shape,
        input_output_aliases=aliases,
        cost_estimate=matmul_cost(rows, len(pairs) * depth, width, width // tn),
        compiler_params=pltpu.CompilerParams(vmem_limit_bytes=FAR_VMEM * MIB),
    )(core, *args)


FAR_VMEM = 28


def solution(mesh):
    across = [(0, 2), (2, 0), (1, 3), (3, 1)]
    beside = [(0, 1), (1, 0), (2, 3), (3, 2)]

    def local_product(a_blk, b_blk):
        depth = b_blk.shape[0]
        row_id = lax.axis_index("row")
        core = lax.rem(row_id, 2).astype(jnp.int32).reshape(1)
        aligned = lax.div(row_id, 2) == lax.axis_index("col")
        starts = []
        x_own = []
        begin = 0
        for width, part, parts in PIECES:
            starts.append(begin)
            rows = depth // parts
            piece = lax.slice(b_blk, (part * rows, begin), ((part + 1) * rows, begin + width))
            x_own.append(lax.ppermute(piece, "row", across))
            if part == parts - 1:
                begin += width
        a_recv = lax.ppermute(a_blk, "col", [(0, 1), (1, 0)])
        b_pair = lax.ppermute(b_blk, "row", beside)
        a_near = jnp.where(aligned, a_blk, a_recv)
        a_far = jnp.where(aligned, a_recv, a_blk)
        c = None
        half = None
        for j, (width, part, parts) in enumerate(PIECES):
            x = x_own[j]
            if half is not None:
                x, half = lax.optimization_barrier((x, half))
            elif j:
                x, c = lax.optimization_barrier((x, c))
            x_pair = lax.ppermute(x, "row", beside)
            if j < TAIL:
                c = whole_product(core, a_near, a_far, b_blk, b_pair, x, x_pair, c, starts[j])
            elif part < parts - 1:
                half = far_product(core, a_far, x, x_pair, sums, starts[j] - starts[TAIL], part, parts, None, starts[j])
            elif half is not None:
                half = far_product(core, a_far, x, None, half, 0, part, parts, None, starts[j])
                c = far_product(core, a_far, None, x_pair, half, 0, part, parts, c, starts[j])
                half = None
            else:
                c = far_product(core, a_far, x, x_pair, sums, starts[j] - starts[TAIL], part, parts, c, starts[j])
            if j == NEAR_AFTER:
                core, c = lax.optimization_barrier((core, c))
                sums = near_sums(core, a_near, b_blk, b_pair, starts[TAIL])
        return c

    return jax.shard_map(
        local_product,
        mesh=mesh,
        in_specs=(P(("dp", "row"), "col"), P("row", "col")),
        out_specs=P(("dp", "row"), "col"),
        check_vma=False,
    )
```

```python
import functools

import jax
import jax.numpy as jnp
from jax import lax
from jax.experimental import pallas as pl
from jax.experimental.pallas import tpu as pltpu
from jax.sharding import PartitionSpec as P


PIECES = (
    (128, 0, 1, 1), (896, 0, 1, 1), (2560, 0, 1, 1), (2560, 0, 1, 1), (2560, 0, 1, 1), (2048, 0, 1, 1),
    (1536, 0, 1, 1), (1024, 0, 1, 1), (512, 0, 1, 1), (256, 0, 1, 1), (256, 0, 2, 4), (256, 2, 3, 4), (256, 3, 4, 4),
)
TAIL = 7
LATE = 9
NEAR_AFTER = 4
MIB = 1024 * 1024


def matmul_cost(rows, depth, width, tiles):
    return pl.CostEstimate(
        flops=2 * rows * depth * width,
        bytes_accessed=2 * (rows * depth * tiles + depth * width + rows * width),
        transcendentals=0,
    )


def tile_of(start, width, most=512):
    for tn in (512, 256, 128):
        if tn <= most and start % tn == 0 and width % tn == 0:
            return tn


def whole_body(a0, a1, a2, a3, b0, b1, b2, b3, *rest):
    c_ref = rest[-1]
    total = jnp.dot(a0[...], b0[...], preferred_element_type=jnp.float32)
    total += jnp.dot(a1[...], b1[...], preferred_element_type=jnp.float32)
    total += jnp.dot(a2[...], b2[...], preferred_element_type=jnp.float32)
    total += jnp.dot(a3[...], b3[...], preferred_element_type=jnp.float32)
    c_ref[...] = total.astype(c_ref.dtype)


def whole_product(a_parts, b_own, b_pair, x_own, x_pair, c_prev, start, tm=512):
    rows, depth = a_parts[0].shape
    columns = b_own.shape[1]
    width = x_own.shape[1]
    tn = tile_of(start, width)
    first = start // tn
    b_whole = pl.BlockSpec((depth, tn), lambda n, m: (0, first + n))
    b_piece = pl.BlockSpec((depth, tn), lambda n, m: (0, n))
    in_specs = [pl.BlockSpec((tm, depth), lambda n, m: (m, 0))] * 4 + [b_whole, b_whole, b_piece, b_piece]
    args = [*a_parts, b_own, b_pair, x_own, x_pair]
    aliases = {}
    if c_prev is not None:
        in_specs.append(pl.BlockSpec(memory_space=pl.ANY))
        aliases = {len(args): 0}
        args.append(c_prev)
    return pl.pallas_call(
        whole_body,
        grid=(width // tn, rows // tm),
        in_specs=in_specs,
        out_specs=pl.BlockSpec((tm, tn), lambda n, m: (m, first + n)),
        out_shape=jax.ShapeDtypeStruct((rows, columns), jnp.bfloat16),
        input_output_aliases=aliases,
        cost_estimate=matmul_cost(rows, 4 * depth, width, width // tn),
        compiler_params=pltpu.CompilerParams(vmem_limit_bytes=62 * MIB),
    )(*args)


def near_body(a0, a1, b0, b1, s_ref):
    s_ref[...] = jnp.dot(a0[...], b0[...], preferred_element_type=jnp.float32)
    s_ref[...] += jnp.dot(a1[...], b1[...], preferred_element_type=jnp.float32)


def near_sums(a_parts, b_own, b_pair, start, tm=512, tn=512):
    rows, depth = a_parts[0].shape
    width = b_own.shape[1] - start
    first = start // tn
    b_whole = pl.BlockSpec((depth, tn), lambda n, m: (0, first + n))
    return pl.pallas_call(
        near_body,
        grid=(width // tn, rows // tm),
        in_specs=[pl.BlockSpec((tm, depth), lambda n, m: (m, 0))] * 2 + [b_whole, b_whole],
        out_specs=pl.BlockSpec((tm, tn), lambda n, m: (m, n)),
        out_shape=jax.ShapeDtypeStruct((rows, width), jnp.float32),
        cost_estimate=matmul_cost(rows, 2 * depth, width, width // tn),
        compiler_params=pltpu.CompilerParams(vmem_limit_bytes=62 * MIB),
        name="near",
    )(*a_parts, b_own, b_pair)


def far_body(count, *refs):
    a_refs, b_refs = refs[:count], refs[count : 2 * count]
    s_ref, out_ref = refs[2 * count], refs[-1]
    total = s_ref[...]
    for a_ref, b_ref in zip(a_refs, b_refs):
        total += jnp.dot(a_ref[...], b_ref[...], preferred_element_type=jnp.float32)
    out_ref[...] = total.astype(out_ref.dtype)


def far_product(pairs, first_row, sums, sums_start, c_prev, start, tm=1024):
    rows = pairs[0][0].shape[0]
    depth, width = pairs[0][1].shape
    tn = tile_of(start, width, 256)
    first = start // tn
    sums_first = sums_start // tn
    a_column = first_row // depth
    in_specs = [pl.BlockSpec((tm, depth), lambda n, m: (m, a_column))] * len(pairs)
    in_specs += [pl.BlockSpec((depth, tn), lambda n, m: (0, n))] * len(pairs)
    in_specs.append(pl.BlockSpec((tm, tn), lambda n, m: (m, sums_first + n)))
    args = [a for a, _ in pairs] + [x for _, x in pairs] + [sums]
    if c_prev is None:
        out_specs = pl.BlockSpec((tm, tn), lambda n, m: (m, n))
        out_shape = jax.ShapeDtypeStruct((rows, width), jnp.float32)
        aliases = {len(args) - 1: 0} if sums.shape == (rows, width) else {}
    else:
        in_specs.append(pl.BlockSpec(memory_space=pl.ANY))
        aliases = {len(args): 0}
        args.append(c_prev)
        out_specs = pl.BlockSpec((tm, tn), lambda n, m: (m, first + n))
        out_shape = jax.ShapeDtypeStruct(c_prev.shape, c_prev.dtype)
    return pl.pallas_call(
        functools.partial(far_body, len(pairs)),
        grid=(width // tn, rows // tm),
        in_specs=in_specs,
        out_specs=out_specs,
        out_shape=out_shape,
        input_output_aliases=aliases,
        cost_estimate=matmul_cost(rows, len(pairs) * depth, width, width // tn),
        compiler_params=pltpu.CompilerParams(vmem_limit_bytes=FAR_VMEM * MIB),
    )(*args)


FAR_VMEM = 28


def solution(mesh):
    across = [(0, 2), (2, 0), (1, 3), (3, 1)]
    beside = [(0, 1), (1, 0), (2, 3), (3, 2)]
    count = len(PIECES)

    def local_product(a_blk, b_blk):
        depth = b_blk.shape[0]
        row_id = lax.axis_index("row")
        first_core = lax.rem(row_id, 2) == 0
        aligned = lax.div(row_id, 2) == lax.axis_index("col")

        starts = []
        begin = 0
        for width, _, end, parts in PIECES:
            starts.append(begin)
            if end == parts:
                begin += width

        def send(j, block):
            width, lo, hi, parts = PIECES[j]
            rows = depth // parts
            piece = lax.slice(block, (lo * rows, starts[j]), (hi * rows, starts[j] + width))
            return lax.ppermute(piece, "row", across)

        x_own = [send(j, b_blk) for j in range(LATE)]
        a_recv = lax.ppermute(a_blk, "col", [(0, 1), (1, 0)])
        b_pair = lax.ppermute(b_blk, "row", beside)
        a_near = []
        a_far = []
        for side in (True, False):
            mine = first_core == side
            halves = [jnp.where(mine, a[:, :depth], a[:, depth:]) for a in (a_blk, a_recv)]
            a_near.append(jnp.where(aligned, halves[0], halves[1]))
            a_far.append(jnp.where(aligned, halves[1], halves[0]))
        c = None
        sums = None
        for j, (width, lo, hi, parts) in enumerate(PIECES):
            if j == LATE - 2:
                b_late, c = lax.optimization_barrier((b_blk, c))
                x_own += [send(i, b_late) for i in range(LATE, count)]
            x = x_own[j]
            if j >= TAIL and lo > 0:
                x, half = lax.optimization_barrier((x, half))
            elif j:
                x, c = lax.optimization_barrier((x, c))
            x_pair = lax.ppermute(x, "row", beside)
            if j < TAIL:
                c = whole_product(a_near + a_far, b_blk, b_pair, x, x_pair, c, starts[j])
            else:
                row = lo * (depth // parts)
                if lo == 0:
                    half, offset = sums, starts[j] - starts[TAIL]
                pairs = [(a_far[0], x), (a_far[1], x_pair)]
                if j == count - 1:
                    half = far_product(pairs[:1], row, half, offset, None, starts[j])
                    pairs = pairs[1:]
                if hi == parts:
                    c = far_product(pairs, row, half, offset, c, starts[j])
                else:
                    half = far_product(pairs, row, half, offset, None, starts[j])
                    offset = 0
            if j == NEAR_AFTER:
                a_near[0], c = lax.optimization_barrier((a_near[0], c))
                sums = near_sums(a_near, b_blk, b_pair, starts[TAIL])
        return c

    return jax.shard_map(
        local_product,
        mesh=mesh,
        in_specs=(P(("dp", "row"), "col"), P("row", "col")),
        out_specs=P(("dp", "row"), "col"),
        check_vma=False,
    )
```

```python
import functools

import jax
import jax.numpy as jnp
from jax import lax
from jax.experimental import pallas as pl
from jax.experimental.pallas import tpu as pltpu
from jax.sharding import PartitionSpec as P


PIECES = (
    (14080, 256, 0, 2, 8),
    (0, 256, 0, 1, 1), (256, 768, 0, 1, 1), (1024, 2560, 0, 1, 1), (3584, 2560, 0, 1, 1), (6144, 2560, 0, 1, 1),
    (8704, 2048, 0, 1, 1), (10752, 1536, 0, 1, 1),
    (12288, 1024, 0, 1, 1), (13312, 512, 0, 1, 1), (13824, 256, 0, 1, 1),
    (14080, 256, 2, 4, 8), (14080, 256, 4, 6, 8), (14080, 256, 6, 7, 8), (14080, 256, 7, 8, 8),
)
TAIL = 8
LATE = 10
LATEST = 13
NEAR_AFTER = 5
MIB = 1024 * 1024


def matmul_cost(rows, depth, width, tiles):
    return pl.CostEstimate(
        flops=2 * rows * depth * width,
        bytes_accessed=2 * (rows * depth * tiles + depth * width + rows * width),
        transcendentals=0,
    )


def tile_of(start, width, most=512):
    for tn in (512, 256, 128):
        if tn <= most and start % tn == 0 and width % tn == 0:
            return tn


def whole_body(a0, a1, a2, a3, b0, b1, b2, b3, *rest):
    c_ref = rest[-1]
    total = jnp.dot(a0[...], b0[...], preferred_element_type=jnp.float32)
    total += jnp.dot(a1[...], b1[...], preferred_element_type=jnp.float32)
    total += jnp.dot(a2[...], b2[...], preferred_element_type=jnp.float32)
    total += jnp.dot(a3[...], b3[...], preferred_element_type=jnp.float32)
    c_ref[...] = total.astype(c_ref.dtype)


def whole_product(a_parts, b_own, b_pair, x_own, x_pair, c_prev, start, tm=512):
    rows, depth = a_parts[0].shape
    columns = b_own.shape[1]
    width = x_own.shape[1]
    tn = tile_of(start, width)
    first = start // tn
    b_whole = pl.BlockSpec((depth, tn), lambda n, m: (0, first + n))
    b_piece = pl.BlockSpec((depth, tn), lambda n, m: (0, n))
    in_specs = [pl.BlockSpec((tm, depth), lambda n, m: (m, 0))] * 4 + [b_whole, b_whole, b_piece, b_piece]
    args = [*a_parts, b_own, b_pair, x_own, x_pair]
    aliases = {}
    if c_prev is not None:
        in_specs.append(pl.BlockSpec(memory_space=pl.ANY))
        aliases = {len(args): 0}
        args.append(c_prev)
    return pl.pallas_call(
        whole_body,
        grid=(width // tn, rows // tm),
        in_specs=in_specs,
        out_specs=pl.BlockSpec((tm, tn), lambda n, m: (m, first + n)),
        out_shape=jax.ShapeDtypeStruct((rows, columns), jnp.bfloat16),
        input_output_aliases=aliases,
        cost_estimate=matmul_cost(rows, 4 * depth, width, width // tn),
        compiler_params=pltpu.CompilerParams(vmem_limit_bytes=62 * MIB),
    )(*args)


def near_body(a0, a1, b0, b1, s_ref):
    s_ref[...] = jnp.dot(a0[...], b0[...], preferred_element_type=jnp.float32)
    s_ref[...] += jnp.dot(a1[...], b1[...], preferred_element_type=jnp.float32)


def near_sums(a_parts, b_own, b_pair, start, tm=512, tn=512):
    rows, depth = a_parts[0].shape
    width = b_own.shape[1] - start
    first = start // tn
    b_whole = pl.BlockSpec((depth, tn), lambda n, m: (0, first + n))
    return pl.pallas_call(
        near_body,
        grid=(width // tn, rows // tm),
        in_specs=[pl.BlockSpec((tm, depth), lambda n, m: (m, 0))] * 2 + [b_whole, b_whole],
        out_specs=pl.BlockSpec((tm, tn), lambda n, m: (m, n)),
        out_shape=jax.ShapeDtypeStruct((rows, width), jnp.float32),
        cost_estimate=matmul_cost(rows, 2 * depth, width, width // tn),
        compiler_params=pltpu.CompilerParams(vmem_limit_bytes=62 * MIB),
        name="near",
    )(*a_parts, b_own, b_pair)


def far_body(count, *refs):
    a_refs, b_refs = refs[:count], refs[count : 2 * count]
    s_ref, out_ref = refs[2 * count], refs[-1]
    total = s_ref[...]
    for a_ref, b_ref in zip(a_refs, b_refs):
        total += jnp.dot(a_ref[...], b_ref[...], preferred_element_type=jnp.float32)
    out_ref[...] = total.astype(out_ref.dtype)


def far_product(terms, sums, sums_start, c_prev, start, tm=1024):
    rows = terms[0][0].shape[0]
    width = terms[0][1].shape[1]
    tn = tile_of(start, width, 256)
    first = start // tn
    sums_first = sums_start // tn
    in_specs = [
        pl.BlockSpec((tm, x.shape[0]), functools.partial(lambda n, m, k: (m, k), k=row // x.shape[0]))
        for _, x, row in terms
    ]
    in_specs += [pl.BlockSpec((x.shape[0], tn), lambda n, m: (0, n)) for _, x, _ in terms]
    in_specs.append(pl.BlockSpec((tm, tn), lambda n, m: (m, sums_first + n)))
    args = [a for a, _, _ in terms] + [x for _, x, _ in terms] + [sums]
    if c_prev is None:
        out_specs = pl.BlockSpec((tm, tn), lambda n, m: (m, n))
        out_shape = jax.ShapeDtypeStruct((rows, width), jnp.float32)
        aliases = {len(args) - 1: 0} if sums.shape == (rows, width) else {}
    else:
        in_specs.append(pl.BlockSpec(memory_space=pl.ANY))
        aliases = {len(args): 0}
        args.append(c_prev)
        out_specs = pl.BlockSpec((tm, tn), lambda n, m: (m, first + n))
        out_shape = jax.ShapeDtypeStruct(c_prev.shape, c_prev.dtype)
    return pl.pallas_call(
        functools.partial(far_body, len(terms)),
        grid=(width // tn, rows // tm),
        in_specs=in_specs,
        out_specs=out_specs,
        out_shape=out_shape,
        input_output_aliases=aliases,
        cost_estimate=matmul_cost(rows, sum(x.shape[0] for _, x, _ in terms), width, width // tn),
        compiler_params=pltpu.CompilerParams(vmem_limit_bytes=FAR_VMEM * MIB),
    )(*args)


def last_body(start, block, a_ref, x_ref, s_ref, c_prev, c_ref, held, sems):
    rows, width = held.shape
    copies = []
    for i in range(rows // block):
        part = pl.ds(i * block, block)
        total = s_ref[part, :] + jnp.dot(a_ref[part, :], x_ref[...], preferred_element_type=jnp.float32)
        held[part, :] = total.astype(held.dtype)
        copy = pltpu.make_async_copy(held.at[part, :], c_ref.at[part, pl.ds(start, width)], sems.at[i])
        copy.start()
        copies.append(copy)
    for copy in copies:
        copy.wait()


def last_product(a, x, row, sums, c_prev, start, block=512):
    rows = a.shape[0]
    depth, width = x.shape
    return pl.pallas_call(
        functools.partial(last_body, start, block),
        grid=(1,),
        in_specs=[
            pl.BlockSpec((rows, depth), lambda n: (0, row // depth)),
            pl.BlockSpec((depth, width), lambda n: (0, 0)),
            pl.BlockSpec((rows, width), lambda n: (0, 0)),
            pl.BlockSpec(memory_space=pl.ANY),
        ],
        out_specs=pl.BlockSpec(memory_space=pl.ANY),
        out_shape=jax.ShapeDtypeStruct(c_prev.shape, c_prev.dtype),
        scratch_shapes=[pltpu.VMEM((rows, width), c_prev.dtype), pltpu.SemaphoreType.DMA((rows // block,))],
        input_output_aliases={3: 0},
        cost_estimate=matmul_cost(rows, depth, width, 1),
        compiler_params=pltpu.CompilerParams(vmem_limit_bytes=FAR_VMEM * MIB),
        name="last",
    )(a, x, sums, c_prev)


FAR_VMEM = 28


def solution(mesh):
    across = [(0, 3), (3, 0), (1, 2), (2, 1)]
    beside = [(0, 1), (1, 0), (2, 3), (3, 2)]
    count = len(PIECES)

    def local_product(a_blk, b_blk):
        depth = b_blk.shape[0]
        row_id = lax.axis_index("row")
        first_core = lax.rem(row_id, 2) == 0
        aligned = lax.div(row_id, 2) == lax.axis_index("col")
        row_of = [lo * depth // parts for _, _, lo, _, parts in PIECES]

        def send(j, block):
            start, width, lo, hi, parts = PIECES[j]
            rows = depth // parts
            piece = lax.slice(block, (lo * rows, start), (hi * rows, start + width))
            return lax.ppermute(piece, "row", across)

        def pass_on(j):
            return lax.ppermute(x_own[j], "row", beside)

        x_own = [send(j, b_blk) for j in range(LATE)]
        x_pair = [None] * count
        a_recv = lax.ppermute(a_blk, "col", [(0, 1), (1, 0)])
        b_pair = lax.ppermute(b_blk, "row", beside)
        a_near = []
        a_far = []
        for side in (True, False):
            mine = first_core == side
            halves = [jnp.where(mine, a[:, :depth], a[:, depth:]) for a in (a_blk, a_recv)]
            a_near.append(jnp.where(aligned, halves[0], halves[1]))
            a_far.insert(0, jnp.where(aligned, halves[1], halves[0]))
        c = None
        for j in range(1, LATE + 1):
            start = PIECES[j][0]
            if j == LATE - 2:
                b_late, c = lax.optimization_barrier((b_blk, c))
                x_own += [send(i, b_late) for i in range(LATE, LATEST)]
            if j == LATE:
                b_late, c = lax.optimization_barrier((b_blk, c))
                x_own += [send(i, b_late) for i in range(LATEST, count)]
            if j > 1:
                x_own[j], c = lax.optimization_barrier((x_own[j], c))
            x_pair[j] = pass_on(j)
            if j < TAIL:
                c = whole_product(a_near + a_far, b_blk, b_pair, x_own[j], x_pair[j], c, start)
            else:
                terms = [(a_far[0], x_own[j], 0), (a_far[1], x_pair[j], 0)]
                c = far_product(terms, sums, start - PIECES[TAIL][0], c, start)
            if j == 2:
                x_own[0], a_last, c = lax.optimization_barrier((x_own[0], a_far[1], c))
                x_pair[0] = pass_on(0)
                a_last = a_last[:, row_of[-1] :]
                a_last, c = lax.optimization_barrier((a_last, c))
            if j == NEAR_AFTER:
                a_near[0], c = lax.optimization_barrier((a_near[0], c))
                sums = near_sums(a_near, b_blk, b_pair, PIECES[TAIL][0])

        start = PIECES[-1][0]
        both = lambda j: [(a_far[0], x_own[j], row_of[j]), (a_far[1], x_pair[j], row_of[j])]
        j = LATE + 1
        x_own[j], c = lax.optimization_barrier((x_own[j], c))
        x_pair[j] = pass_on(j)
        half = far_product(both(0) + both(j), sums, start - PIECES[TAIL][0], None, start)
        j += 1
        x_own[j], half = lax.optimization_barrier((x_own[j], half))
        x_pair[j] = pass_on(j)
        half = far_product(both(j), half, 0, None, start)
        j += 1
        x_own[j], half = lax.optimization_barrier((x_own[j], half))
        x_pair[j] = pass_on(j)
        j += 1
        x_own[j], x_pair[j - 1] = lax.optimization_barrier((x_own[j], x_pair[j - 1]))
        x_pair[j] = pass_on(j)
        half = far_product(both(j - 1) + both(j)[:1], half, 0, None, start)
        c = last_product(a_last, x_pair[j], 0, half, c, start)
        return c

    return jax.shard_map(
        local_product,
        mesh=mesh,
        in_specs=(P(("dp", "row"), "col"), P("row", "col")),
        out_specs=P(("dp", "row"), "col"),
        check_vma=False,
    )
```

```python
import functools

import jax
import jax.numpy as jnp
from jax import lax
from jax.experimental import pallas as pl
from jax.experimental.pallas import tpu as pltpu
from jax.sharding import PartitionSpec as P


PIECES = (
    (14080, 256, 0, 4),
    (0, 256, 0, 16), (256, 768, 0, 16), (1024, 2560, 0, 16), (3584, 2560, 0, 16), (6144, 2560, 0, 16),
    (8704, 2048, 0, 16), (10752, 1536, 0, 16),
    (12288, 1024, 0, 16), (13312, 512, 0, 16), (13824, 256, 0, 16),
    (14080, 256, 4, 5), (14080, 256, 9, 4), (14080, 256, 13, 3),
)
TAIL = 8
LATE = 10
LATEST = 12
NEAR_AFTER = 5
FAR_VMEM = 24
MIB = 1024 * 1024


def matmul_cost(rows, depth, width, tiles):
    return pl.CostEstimate(
        flops=2 * rows * depth * width,
        bytes_accessed=2 * (rows * depth * tiles + depth * width + rows * width),
        transcendentals=0,
    )


def tile_of(start, width, most=512):
    for tn in (512, 256, 128):
        if tn <= most and start % tn == 0 and width % tn == 0:
            return tn


def whole_body(a0, a1, a2, a3, b0, b1, b2, b3, *rest):
    c_ref = rest[-1]
    total = jnp.dot(a0[...], b0[...], preferred_element_type=jnp.float32)
    total += jnp.dot(a1[...], b1[...], preferred_element_type=jnp.float32)
    total += jnp.dot(a2[...], b2[...], preferred_element_type=jnp.float32)
    total += jnp.dot(a3[...], b3[...], preferred_element_type=jnp.float32)
    c_ref[...] = total.astype(c_ref.dtype)


def whole_product(a_parts, b_own, b_pair, x_own, x_pair, c_prev, start, tm=512):
    rows, depth = a_parts[0].shape
    columns = b_own.shape[1]
    width = x_own.shape[1]
    tn = tile_of(start, width)
    first = start // tn
    b_whole = pl.BlockSpec((depth, tn), lambda n, m: (0, first + n))
    b_piece = pl.BlockSpec((depth, tn), lambda n, m: (0, n))
    in_specs = [pl.BlockSpec((tm, depth), lambda n, m: (m, 0))] * 4 + [b_whole, b_whole, b_piece, b_piece]
    args = [*a_parts, b_own, b_pair, x_own, x_pair]
    aliases = {}
    if c_prev is not None:
        in_specs.append(pl.BlockSpec(memory_space=pl.ANY))
        aliases = {len(args): 0}
        args.append(c_prev)
    return pl.pallas_call(
        whole_body,
        grid=(width // tn, rows // tm),
        in_specs=in_specs,
        out_specs=pl.BlockSpec((tm, tn), lambda n, m: (m, first + n)),
        out_shape=jax.ShapeDtypeStruct((rows, columns), jnp.bfloat16),
        input_output_aliases=aliases,
        cost_estimate=matmul_cost(rows, 4 * depth, width, width // tn),
        compiler_params=pltpu.CompilerParams(vmem_limit_bytes=62 * MIB),
    )(*args)


def near_body(a0, a1, b0, b1, *rest):
    s_ref = rest[-1]
    total = jnp.dot(a0[...], b0[...], preferred_element_type=jnp.float32)
    total += jnp.dot(a1[...], b1[...], preferred_element_type=jnp.float32)
    if len(rest) > 1:
        total += rest[0][...]
    s_ref[...] = total


def near_sums(a_parts, b_own, b_pair, more, start, width, tm=512, tn=256):
    rows, depth = a_parts[0].shape
    first = start // tn
    b_whole = pl.BlockSpec((depth, tn), lambda n, m: (0, first + n))
    in_specs = [pl.BlockSpec((tm, depth), lambda n, m: (m, 0))] * 2 + [b_whole, b_whole]
    args = [*a_parts, b_own, b_pair]
    if more is not None:
        in_specs.append(pl.BlockSpec((tm, tn), lambda n, m: (m, n)))
        args.append(more)
    return pl.pallas_call(
        near_body,
        grid=(width // tn, rows // tm),
        in_specs=in_specs,
        out_specs=pl.BlockSpec((tm, tn), lambda n, m: (m, n)),
        out_shape=jax.ShapeDtypeStruct((rows, width), jnp.float32),
        cost_estimate=matmul_cost(rows, 2 * depth, width, width // tn),
        compiler_params=pltpu.CompilerParams(vmem_limit_bytes=62 * MIB),
    )(*args)


def far_body(a_of, columns, summed, *refs):
    count = len(a_of)
    x_refs = refs[max(a_of) + 1 :]
    total = x_refs[count][...] if summed else None
    for which, column, x_ref in zip(a_of, columns, x_refs):
        depth = x_ref.shape[0]
        product = jnp.dot(
            refs[which][:, column : column + depth], x_ref[...], preferred_element_type=jnp.float32
        )
        total = product if total is None else total + product
    refs[-1][...] = total.astype(refs[-1].dtype)


def far_product(a_far, terms, sums, sums_start, c_prev, start, tm=1024):
    rows, depth = a_far[0].shape
    width = terms[0][1].shape[1]
    tn = tile_of(start, width, 256)
    first = start // tn
    sums_first = sums_start // tn
    used = sorted({i for i, _, _ in terms})
    args = [a_far[i] for i in used] + [x for _, x, _ in terms]
    in_specs = [pl.BlockSpec((tm, depth), lambda n, m: (m, 0)) for _ in used]
    in_specs += [pl.BlockSpec((x.shape[0], tn), lambda n, m: (0, n)) for _, x, _ in terms]
    aliases = {}
    if sums is not None:
        in_specs.append(pl.BlockSpec((tm, tn), lambda n, m: (m, sums_first + n)))
        args.append(sums)
    if c_prev is None:
        out_specs = pl.BlockSpec((tm, tn), lambda n, m: (m, n))
        out_shape = jax.ShapeDtypeStruct((rows, width), jnp.float32)
        if sums is not None and sums.shape == (rows, width):
            aliases = {len(args) - 1: 0}
    else:
        in_specs.append(pl.BlockSpec(memory_space=pl.ANY))
        aliases = {len(args): 0}
        args.append(c_prev)
        out_specs = pl.BlockSpec((tm, tn), lambda n, m: (m, first + n))
        out_shape = jax.ShapeDtypeStruct(c_prev.shape, c_prev.dtype)
    return pl.pallas_call(
        functools.partial(
            far_body, [used.index(i) for i, _, _ in terms], [row for _, _, row in terms], sums is not None
        ),
        grid=(width // tn, rows // tm),
        in_specs=in_specs,
        out_specs=out_specs,
        out_shape=out_shape,
        input_output_aliases=aliases,
        cost_estimate=matmul_cost(rows, sum(x.shape[0] for _, x, _ in terms), width, width // tn),
        compiler_params=pltpu.CompilerParams(vmem_limit_bytes=FAR_VMEM * MIB),
    )(*args)


def last_body(start, block, a_ref, x_ref, s_ref, c_prev, c_ref, held, sems):
    rows, width = held.shape
    copies = []
    for i in range(rows // block):
        part = pl.ds(i * block, block)
        total = s_ref[part, :] + jnp.dot(a_ref[part, :], x_ref[...], preferred_element_type=jnp.float32)
        held[part, :] = total.astype(held.dtype)
        copy = pltpu.make_async_copy(held.at[part, :], c_ref.at[part, pl.ds(start, width)], sems.at[i])
        copy.start()
        copies.append(copy)
    for copy in copies:
        copy.wait()


def last_product(a, x, sums, c_prev, start, block=512):
    rows = a.shape[0]
    depth, width = x.shape
    return pl.pallas_call(
        functools.partial(last_body, start, block),
        grid=(1,),
        in_specs=[
            pl.BlockSpec((rows, depth), lambda n: (0, 0)),
            pl.BlockSpec((depth, width), lambda n: (0, 0)),
            pl.BlockSpec((rows, width), lambda n: (0, 0)),
            pl.BlockSpec(memory_space=pl.ANY),
        ],
        out_specs=pl.BlockSpec(memory_space=pl.ANY),
        out_shape=jax.ShapeDtypeStruct(c_prev.shape, c_prev.dtype),
        scratch_shapes=[pltpu.VMEM((rows, width), c_prev.dtype), pltpu.SemaphoreType.DMA((rows // block,))],
        input_output_aliases={3: 0},
        cost_estimate=matmul_cost(rows, depth, width, 1),
        compiler_params=pltpu.CompilerParams(vmem_limit_bytes=FAR_VMEM * MIB),
        name="last",
    )(a, x, sums, c_prev)


def solution(mesh):
    across = [(0, 3), (3, 0), (1, 2), (2, 1)]
    beside = [(0, 1), (1, 0), (2, 3), (3, 2)]
    count = len(PIECES)
    last = count - 1

    def local_product(a_blk, b_blk):
        depth = b_blk.shape[0]
        row_id = lax.axis_index("row")
        first_core = lax.rem(row_id, 2) == 0
        aligned = lax.div(row_id, 2) == lax.axis_index("col")
        row_of = [row * depth // 16 for _, _, row, _ in PIECES]
        x_own = [None] * count
        x_pair = [None] * count

        def send(j, block):
            start, width, _, rows = PIECES[j]
            piece = lax.slice(block, (row_of[j], start), (row_of[j] + rows * depth // 16, start + width))
            x_own[j] = lax.ppermute(piece, "row", across)

        def pass_on(j, after):
            x_own[j], after = lax.optimization_barrier((x_own[j], after))
            x_pair[j] = lax.ppermute(x_own[j], "row", beside)
            return after

        def both(j):
            return [(0, x_own[j], row_of[j]), (1, x_pair[j], row_of[j])]

        for j in range(LATE):
            send(j, b_blk)
        a_recv = lax.ppermute(a_blk, "col", [(0, 1), (1, 0)])
        b_pair = lax.ppermute(b_blk, "row", beside)
        x_pair[0] = lax.ppermute(x_own[0], "row", beside)
        a_near = []
        a_far = []
        for side in (True, False):
            mine = first_core == side
            halves = [jnp.where(mine, a[:, :depth], a[:, depth:]) for a in (a_blk, a_recv)]
            a_near.append(jnp.where(aligned, halves[0], halves[1]))
            a_far.insert(0, jnp.where(aligned, halves[1], halves[0]))
        tail = PIECES[TAIL][0]
        end = PIECES[last][0]
        half = far_product(a_far, both(0), None, 0, None, end)
        c = None
        for j in range(1, LATE + 1):
            start = PIECES[j][0]
            if j == LATE - 2:
                b_late, c = lax.optimization_barrier((b_blk, c))
                for i in range(LATE, LATEST):
                    send(i, b_late)
            if j == LATE:
                b_late, c = lax.optimization_barrier((b_blk, c))
                for i in range(LATEST, count):
                    send(i, b_late)
            if j == 1:
                half = pass_on(j, half)
            else:
                c = pass_on(j, c)
            if j < TAIL:
                c = whole_product(a_near + a_far, b_blk, b_pair, x_own[j], x_pair[j], c, start)
            else:
                c = far_product(a_far, both(j), sums, start - tail, c, start)
            if j == 2:
                a_last, c = lax.optimization_barrier((a_far[1], c))
                a_last = a_last[:, row_of[last] :]
                a_last, c = lax.optimization_barrier((a_last, c))
            if j == NEAR_AFTER:
                a_near[0], c = lax.optimization_barrier((a_near[0], c))
                sums = near_sums(a_near, b_blk, b_pair, None, tail, end - tail)
                half = near_sums(a_near, b_blk, b_pair, half, end, b_blk.shape[1] - end)

        for j in range(LATE + 1, last):
            c = pass_on(j, c)
            half = far_product(a_far, both(j), half, 0, None, end)
            half, c = lax.optimization_barrier((half, c))
        half = pass_on(last, half)
        half = far_product(a_far, both(last)[:1], half, 0, None, end)
        c = last_product(a_last, x_pair[last], half, c, end)
        return c

    return jax.shard_map(
        local_product,
        mesh=mesh,
        in_specs=(P(("dp", "row"), "col"), P("row", "col")),
        out_specs=P(("dp", "row"), "col"),
        check_vma=False,
    )
```

```python
import functools

import jax
import jax.numpy as jnp
from jax import lax
from jax.experimental import pallas as pl
from jax.experimental.pallas import tpu as pltpu
from jax.sharding import PartitionSpec as P


PIECES = (
    (14080, 256, 0, 3),
    (0, 256, 0, 16), (256, 768, 0, 16), (1024, 2560, 0, 16), (3584, 2560, 0, 16), (6144, 2560, 0, 16),
    (8704, 2048, 0, 16), (10752, 1536, 0, 16),
    (12288, 1024, 0, 16), (13312, 512, 0, 16), (13824, 256, 0, 16),
    (14080, 256, 3, 6), (14080, 256, 9, 4), (14080, 256, 13, 3),
)
TAIL = 8
LATE = 10
LATEST = 12
NEAR_AFTER = 5
FAR_VMEM = 24
MIB = 1024 * 1024


def matmul_cost(rows, depth, width, tiles):
    return pl.CostEstimate(
        flops=2 * rows * depth * width,
        bytes_accessed=2 * (rows * depth * tiles + depth * width + rows * width),
        transcendentals=0,
    )


def tile_of(start, width, most=512):
    for tn in (512, 256, 128):
        if tn <= most and start % tn == 0 and width % tn == 0:
            return tn


def whole_body(a0, a1, a2, a3, b0, b1, b2, b3, *rest):
    c_ref = rest[-1]
    total = jnp.dot(a0[...], b0[...], preferred_element_type=jnp.float32)
    total += jnp.dot(a1[...], b1[...], preferred_element_type=jnp.float32)
    total += jnp.dot(a2[...], b2[...], preferred_element_type=jnp.float32)
    total += jnp.dot(a3[...], b3[...], preferred_element_type=jnp.float32)
    c_ref[...] = total.astype(c_ref.dtype)


def whole_product(a_parts, b_own, b_pair, x_own, x_pair, c_prev, start, tm=512):
    rows, depth = a_parts[0].shape
    columns = b_own.shape[1]
    width = x_own.shape[1]
    tn = tile_of(start, width)
    first = start // tn
    b_whole = pl.BlockSpec((depth, tn), lambda n, m: (0, first + n))
    b_piece = pl.BlockSpec((depth, tn), lambda n, m: (0, n))
    in_specs = [pl.BlockSpec((tm, depth), lambda n, m: (m, 0))] * 4 + [b_whole, b_whole, b_piece, b_piece]
    args = [*a_parts, b_own, b_pair, x_own, x_pair]
    aliases = {}
    if c_prev is not None:
        in_specs.append(pl.BlockSpec(memory_space=pl.ANY))
        aliases = {len(args): 0}
        args.append(c_prev)
    return pl.pallas_call(
        whole_body,
        grid=(width // tn, rows // tm),
        in_specs=in_specs,
        out_specs=pl.BlockSpec((tm, tn), lambda n, m: (m, first + n)),
        out_shape=jax.ShapeDtypeStruct((rows, columns), jnp.bfloat16),
        input_output_aliases=aliases,
        cost_estimate=matmul_cost(rows, 4 * depth, width, width // tn),
        compiler_params=pltpu.CompilerParams(vmem_limit_bytes=62 * MIB),
    )(*args)


def near_body(a0, a1, b0, b1, *rest):
    s_ref = rest[-1]
    total = jnp.dot(a0[...], b0[...], preferred_element_type=jnp.float32)
    total += jnp.dot(a1[...], b1[...], preferred_element_type=jnp.float32)
    if len(rest) > 1:
        total += rest[0][...]
    s_ref[...] = total


def near_sums(a_parts, b_own, b_pair, more, start, width, tm=512, tn=256):
    rows, depth = a_parts[0].shape
    first = start // tn
    b_whole = pl.BlockSpec((depth, tn), lambda n, m: (0, first + n))
    in_specs = [pl.BlockSpec((tm, depth), lambda n, m: (m, 0))] * 2 + [b_whole, b_whole]
    args = [*a_parts, b_own, b_pair]
    if more is not None:
        in_specs.append(pl.BlockSpec((tm, tn), lambda n, m: (m, n)))
        args.append(more)
    return pl.pallas_call(
        near_body,
        grid=(width // tn, rows // tm),
        in_specs=in_specs,
        out_specs=pl.BlockSpec((tm, tn), lambda n, m: (m, n)),
        out_shape=jax.ShapeDtypeStruct((rows, width), jnp.float32),
        cost_estimate=matmul_cost(rows, 2 * depth, width, width // tn),
        compiler_params=pltpu.CompilerParams(vmem_limit_bytes=62 * MIB),
    )(*args)


def far_body(a_of, columns, summed, *refs):
    count = len(a_of)
    x_refs = refs[max(a_of) + 1 :]
    total = x_refs[count][...] if summed else None
    for which, column, x_ref in zip(a_of, columns, x_refs):
        depth = x_ref.shape[0]
        product = jnp.dot(
            refs[which][:, column : column + depth], x_ref[...], preferred_element_type=jnp.float32
        )
        total = product if total is None else total + product
    refs[-1][...] = total.astype(refs[-1].dtype)


def far_product(a_far, terms, sums, sums_start, c_prev, start, tm=1024):
    rows, depth = a_far[0].shape
    width = terms[0][1].shape[1]
    tn = tile_of(start, width, 256)
    first = start // tn
    sums_first = sums_start // tn
    used = sorted({i for i, _, _ in terms})
    args = [a_far[i] for i in used] + [x for _, x, _ in terms]
    in_specs = [pl.BlockSpec((tm, depth), lambda n, m: (m, 0)) for _ in used]
    in_specs += [pl.BlockSpec((x.shape[0], tn), lambda n, m: (0, n)) for _, x, _ in terms]
    aliases = {}
    if sums is not None:
        in_specs.append(pl.BlockSpec((tm, tn), lambda n, m: (m, sums_first + n)))
        args.append(sums)
    if c_prev is None:
        out_specs = pl.BlockSpec((tm, tn), lambda n, m: (m, n))
        out_shape = jax.ShapeDtypeStruct((rows, width), jnp.float32)
        if sums is not None and sums.shape == (rows, width):
            aliases = {len(args) - 1: 0}
    else:
        in_specs.append(pl.BlockSpec(memory_space=pl.ANY))
        aliases = {len(args): 0}
        args.append(c_prev)
        out_specs = pl.BlockSpec((tm, tn), lambda n, m: (m, first + n))
        out_shape = jax.ShapeDtypeStruct(c_prev.shape, c_prev.dtype)
    return pl.pallas_call(
        functools.partial(
            far_body, [used.index(i) for i, _, _ in terms], [row for _, _, row in terms], sums is not None
        ),
        grid=(width // tn, rows // tm),
        in_specs=in_specs,
        out_specs=out_specs,
        out_shape=out_shape,
        input_output_aliases=aliases,
        cost_estimate=matmul_cost(rows, sum(x.shape[0] for _, x, _ in terms), width, width // tn),
        compiler_params=pltpu.CompilerParams(vmem_limit_bytes=FAR_VMEM * MIB),
    )(*args)


def last_body(start, block, a_ref, x_ref, s_ref, c_prev, c_ref, held, sems):
    rows, width = held.shape
    copies = []
    for i in range(rows // block):
        part = pl.ds(i * block, block)
        total = s_ref[part, :] + jnp.dot(a_ref[part, :], x_ref[...], preferred_element_type=jnp.float32)
        held[part, :] = total.astype(held.dtype)
        copy = pltpu.make_async_copy(held.at[part, :], c_ref.at[part, pl.ds(start, width)], sems.at[i])
        copy.start()
        copies.append(copy)
    for copy in copies:
        copy.wait()


def last_product(a, x, sums, c_prev, start, block=512):
    rows = a.shape[0]
    depth, width = x.shape
    return pl.pallas_call(
        functools.partial(last_body, start, block),
        grid=(1,),
        in_specs=[
            pl.BlockSpec((rows, depth), lambda n: (0, 0)),
            pl.BlockSpec((depth, width), lambda n: (0, 0)),
            pl.BlockSpec((rows, width), lambda n: (0, 0)),
            pl.BlockSpec(memory_space=pl.ANY),
        ],
        out_specs=pl.BlockSpec(memory_space=pl.ANY),
        out_shape=jax.ShapeDtypeStruct(c_prev.shape, c_prev.dtype),
        scratch_shapes=[pltpu.VMEM((rows, width), c_prev.dtype), pltpu.SemaphoreType.DMA((rows // block,))],
        input_output_aliases={3: 0},
        cost_estimate=matmul_cost(rows, depth, width, 1),
        compiler_params=pltpu.CompilerParams(vmem_limit_bytes=FAR_VMEM * MIB),
        name="last",
    )(a, x, sums, c_prev)


def solution(mesh):
    across = [(0, 3), (3, 0), (1, 2), (2, 1)]
    beside = [(0, 1), (1, 0), (2, 3), (3, 2)]
    count = len(PIECES)
    last = count - 1

    def local_product(a_blk, b_blk):
        depth = b_blk.shape[0]
        row_id = lax.axis_index("row")
        first_core = lax.rem(row_id, 2) == 0
        aligned = lax.div(row_id, 2) == lax.axis_index("col")
        row_of = [row * depth // 16 for _, _, row, _ in PIECES]
        x_own = [None] * count
        x_pair = [None] * count

        def send(j, block):
            start, width, _, rows = PIECES[j]
            piece = lax.slice(block, (row_of[j], start), (row_of[j] + rows * depth // 16, start + width))
            x_own[j] = lax.ppermute(piece, "row", across)

        def pass_on(j, after):
            x_own[j], after = lax.optimization_barrier((x_own[j], after))
            x_pair[j] = lax.ppermute(x_own[j], "row", beside)
            return after

        def both(j):
            return [(0, x_own[j], row_of[j]), (1, x_pair[j], row_of[j])]

        for j in range(LATE):
            send(j, b_blk)
        a_recv = lax.ppermute(a_blk, "col", [(0, 1), (1, 0)])
        b_pair = lax.ppermute(b_blk, "row", beside)
        x_pair[0] = lax.ppermute(x_own[0], "row", beside)
        a_near = []
        a_far = []
        for side in (True, False):
            mine = first_core == side
            halves = [jnp.where(mine, a[:, :depth], a[:, depth:]) for a in (a_blk, a_recv)]
            a_near.append(jnp.where(aligned, halves[0], halves[1]))
            a_far.insert(0, jnp.where(aligned, halves[1], halves[0]))
        tail = PIECES[TAIL][0]
        before = PIECES[LATE][0]
        end = PIECES[last][0]
        half = far_product(a_far, both(0), None, 0, None, end)
        c = None
        for j in range(1, LATE + 1):
            start = PIECES[j][0]
            if j == LATE - 2:
                b_late, c = lax.optimization_barrier((b_blk, c))
                for i in range(LATE, LATEST):
                    send(i, b_late)
            if j == LATE:
                b_late, c = lax.optimization_barrier((b_blk, c))
                for i in range(LATEST, count):
                    send(i, b_late)
            if j == 1:
                half = pass_on(j, half)
            else:
                c = pass_on(j, c)
            if j < TAIL:
                c = whole_product(a_near + a_far, b_blk, b_pair, x_own[j], x_pair[j], c, start)
            else:
                near, near_start = (sums_before, before) if j == LATE else (sums, tail)
                c = far_product(a_far, both(j), near, start - near_start, c, start)
            if j == 2:
                a_last, c = lax.optimization_barrier((a_far[1], c))
                a_last = a_last[:, row_of[last] :]
                a_last, c = lax.optimization_barrier((a_last, c))
            if j == NEAR_AFTER:
                a_near[0], c = lax.optimization_barrier((a_near[0], c))
                sums = near_sums(a_near, b_blk, b_pair, None, tail, before - tail)
                sums_before = near_sums(a_near, b_blk, b_pair, None, before, end - before)
                half = near_sums(a_near, b_blk, b_pair, half, end, b_blk.shape[1] - end)

        for j in range(LATE + 1, last):
            c = pass_on(j, c)
            half = far_product(a_far, both(j), half, 0, None, end)
            half, c = lax.optimization_barrier((half, c))
        half = pass_on(last, half)
        half = far_product(a_far, both(last)[:1], half, 0, None, end)
        c = last_product(a_last, x_pair[last], half, c, end)
        return c

    return jax.shard_map(
        local_product,
        mesh=mesh,
        in_specs=(P(("dp", "row"), "col"), P("row", "col")),
        out_specs=P(("dp", "row"), "col"),
        check_vma=False,
    )
```

```python
import functools

import jax
import jax.numpy as jnp
from jax import lax
from jax.experimental import pallas as pl
from jax.experimental.pallas import tpu as pltpu
from jax.sharding import PartitionSpec as P


PIECES = (
    (14080, 256, 0, 3),
    (0, 256, 0, 16), (256, 768, 0, 16), (1024, 2560, 0, 16), (3584, 2560, 0, 16), (6144, 2560, 0, 16),
    (8704, 2048, 0, 16), (10752, 1536, 0, 16),
    (12288, 1024, 0, 16), (13312, 512, 0, 16), (13824, 256, 0, 16),
    (14080, 256, 3, 6), (14080, 256, 9, 4), (14080, 256, 13, 3),
)
TAIL = 8
LATE = 10
LATEST = 12
NEAR_AFTER = 5
FAR_VMEM = 24
MIB = 1024 * 1024


def matmul_cost(rows, depth, width, tiles):
    return pl.CostEstimate(
        flops=2 * rows * depth * width,
        bytes_accessed=2 * (rows * depth * tiles + depth * width + rows * width),
        transcendentals=0,
    )


def tile_of(start, width, most=512):
    for tn in (512, 256, 128):
        if tn <= most and start % tn == 0 and width % tn == 0:
            return tn


def whole_body(a0, a1, a2, a3, b0, b1, b2, b3, *rest):
    c_ref = rest[-1]
    total = jnp.dot(a0[...], b0[...], preferred_element_type=jnp.float32)
    total += jnp.dot(a1[...], b1[...], preferred_element_type=jnp.float32)
    total += jnp.dot(a2[...], b2[...], preferred_element_type=jnp.float32)
    total += jnp.dot(a3[...], b3[...], preferred_element_type=jnp.float32)
    c_ref[...] = total.astype(c_ref.dtype)


def whole_product(a_parts, b_own, b_pair, x_own, x_pair, c_prev, start, vmem, tm=512):
    rows, depth = a_parts[0].shape
    columns = b_own.shape[1]
    width = x_own.shape[1]
    tn = tile_of(start, width)
    first = start // tn
    b_whole = pl.BlockSpec((depth, tn), lambda n, m: (0, first + n))
    b_piece = pl.BlockSpec((depth, tn), lambda n, m: (0, n))
    in_specs = [pl.BlockSpec((tm, depth), lambda n, m: (m, 0))] * 4 + [b_whole, b_whole, b_piece, b_piece]
    args = [*a_parts, b_own, b_pair, x_own, x_pair]
    aliases = {}
    if c_prev is not None:
        in_specs.append(pl.BlockSpec(memory_space=pl.ANY))
        aliases = {len(args): 0}
        args.append(c_prev)
    return pl.pallas_call(
        whole_body,
        grid=(width // tn, rows // tm),
        in_specs=in_specs,
        out_specs=pl.BlockSpec((tm, tn), lambda n, m: (m, first + n)),
        out_shape=jax.ShapeDtypeStruct((rows, columns), jnp.bfloat16),
        input_output_aliases=aliases,
        cost_estimate=matmul_cost(rows, 4 * depth, width, width // tn),
        compiler_params=pltpu.CompilerParams(vmem_limit_bytes=vmem * MIB),
    )(*args)


def near_body(a0, a1, b0, b1, *rest):
    s_ref = rest[-1]
    total = jnp.dot(a0[...], b0[...], preferred_element_type=jnp.float32)
    total += jnp.dot(a1[...], b1[...], preferred_element_type=jnp.float32)
    if len(rest) > 1:
        total += rest[0][...]
    s_ref[...] = total


def near_sums(a_parts, b_own, b_pair, more, start, width, tm=512, tn=256):
    rows, depth = a_parts[0].shape
    first = start // tn
    b_whole = pl.BlockSpec((depth, tn), lambda n, m: (0, first + n))
    in_specs = [pl.BlockSpec((tm, depth), lambda n, m: (m, 0))] * 2 + [b_whole, b_whole]
    args = [*a_parts, b_own, b_pair]
    if more is not None:
        in_specs.append(pl.BlockSpec((tm, tn), lambda n, m: (m, n)))
        args.append(more)
    return pl.pallas_call(
        near_body,
        grid=(width // tn, rows // tm),
        in_specs=in_specs,
        out_specs=pl.BlockSpec((tm, tn), lambda n, m: (m, n)),
        out_shape=jax.ShapeDtypeStruct((rows, width), jnp.float32),
        cost_estimate=matmul_cost(rows, 2 * depth, width, width // tn),
        compiler_params=pltpu.CompilerParams(vmem_limit_bytes=62 * MIB),
    )(*args)


def far_body(a_of, columns, summed, *refs):
    count = len(a_of)
    x_refs = refs[max(a_of) + 1 :]
    total = x_refs[count][...] if summed else None
    for which, column, x_ref in zip(a_of, columns, x_refs):
        depth = x_ref.shape[0]
        product = jnp.dot(
            refs[which][:, column : column + depth], x_ref[...], preferred_element_type=jnp.float32
        )
        total = product if total is None else total + product
    refs[-1][...] = total.astype(refs[-1].dtype)


def far_product(a_far, terms, sums, sums_start, c_prev, start, tm=1024):
    rows, depth = a_far[0].shape
    width = terms[0][1].shape[1]
    tn = tile_of(start, width, 256)
    first = start // tn
    sums_first = sums_start // tn
    used = sorted({i for i, _, _ in terms})
    args = [a_far[i] for i in used] + [x for _, x, _ in terms]
    in_specs = [pl.BlockSpec((tm, depth), lambda n, m: (m, 0)) for _ in used]
    in_specs += [pl.BlockSpec((x.shape[0], tn), lambda n, m: (0, n)) for _, x, _ in terms]
    aliases = {}
    if sums is not None:
        in_specs.append(pl.BlockSpec((tm, tn), lambda n, m: (m, sums_first + n)))
        args.append(sums)
    if c_prev is None:
        out_specs = pl.BlockSpec((tm, tn), lambda n, m: (m, n))
        out_shape = jax.ShapeDtypeStruct((rows, width), jnp.float32)
        if sums is not None and sums.shape == (rows, width):
            aliases = {len(args) - 1: 0}
    else:
        in_specs.append(pl.BlockSpec(memory_space=pl.ANY))
        aliases = {len(args): 0}
        args.append(c_prev)
        out_specs = pl.BlockSpec((tm, tn), lambda n, m: (m, first + n))
        out_shape = jax.ShapeDtypeStruct(c_prev.shape, c_prev.dtype)
    return pl.pallas_call(
        functools.partial(
            far_body, [used.index(i) for i, _, _ in terms], [row for _, _, row in terms], sums is not None
        ),
        grid=(width // tn, rows // tm),
        in_specs=in_specs,
        out_specs=out_specs,
        out_shape=out_shape,
        input_output_aliases=aliases,
        cost_estimate=matmul_cost(rows, sum(x.shape[0] for _, x, _ in terms), width, width // tn),
        compiler_params=pltpu.CompilerParams(vmem_limit_bytes=FAR_VMEM * MIB),
    )(*args)


def last_body(start, blocks, a_ref, x_ref, s_ref, c_prev, c_ref, held, sems):
    width = held.shape[1]
    copies = []
    for i, block in enumerate(blocks):
        part = pl.ds(sum(blocks[:i]), block)
        total = s_ref[part, :] + jnp.dot(a_ref[part, :], x_ref[...], preferred_element_type=jnp.float32)
        held[part, :] = total.astype(held.dtype)
        copy = pltpu.make_async_copy(held.at[part, :], c_ref.at[part, pl.ds(start, width)], sems.at[i])
        copy.start()
        copies.append(copy)
    for copy in copies:
        copy.wait()


def last_product(a, x, sums, c_prev, start, eighths=(3, 3, 1, 1)):
    rows = a.shape[0]
    depth, width = x.shape
    return pl.pallas_call(
        functools.partial(last_body, start, [rows // 8 * n for n in eighths]),
        grid=(1,),
        in_specs=[
            pl.BlockSpec((rows, depth), lambda n: (0, 0)),
            pl.BlockSpec((depth, width), lambda n: (0, 0)),
            pl.BlockSpec((rows, width), lambda n: (0, 0)),
            pl.BlockSpec(memory_space=pl.ANY),
        ],
        out_specs=pl.BlockSpec(memory_space=pl.ANY),
        out_shape=jax.ShapeDtypeStruct(c_prev.shape, c_prev.dtype),
        scratch_shapes=[pltpu.VMEM((rows, width), c_prev.dtype), pltpu.SemaphoreType.DMA((len(eighths),))],
        input_output_aliases={3: 0},
        cost_estimate=matmul_cost(rows, depth, width, 1),
        compiler_params=pltpu.CompilerParams(vmem_limit_bytes=FAR_VMEM * MIB),
        name="last",
    )(a, x, sums, c_prev)


def solution(mesh):
    across = [(0, 3), (3, 0), (1, 2), (2, 1)]
    beside = [(0, 1), (1, 0), (2, 3), (3, 2)]
    count = len(PIECES)
    last = count - 1

    def local_product(a_blk, b_blk):
        depth = b_blk.shape[0]
        row_id = lax.axis_index("row")
        first_core = lax.rem(row_id, 2) == 0
        aligned = lax.div(row_id, 2) == lax.axis_index("col")
        row_of = [row * depth // 16 for _, _, row, _ in PIECES]
        x_own = [None] * count
        x_pair = [None] * count

        def send(j, block):
            start, width, _, rows = PIECES[j]
            piece = lax.slice(block, (row_of[j], start), (row_of[j] + rows * depth // 16, start + width))
            x_own[j] = lax.ppermute(piece, "row", across)

        def pass_on(j, after):
            x_own[j], after = lax.optimization_barrier((x_own[j], after))
            x_pair[j] = lax.ppermute(x_own[j], "row", beside)
            return after

        def both(j):
            return [(0, x_own[j], row_of[j]), (1, x_pair[j], row_of[j])]

        for j in range(LATE):
            send(j, b_blk)
        a_recv = lax.ppermute(a_blk, "col", [(0, 1), (1, 0)])
        b_pair = lax.ppermute(b_blk, "row", beside)
        x_pair[0] = lax.ppermute(x_own[0], "row", beside)
        a_near = []
        a_far = []
        for side in (True, False):
            mine = first_core == side
            halves = [jnp.where(mine, a[:, :depth], a[:, depth:]) for a in (a_blk, a_recv)]
            a_near.append(jnp.where(aligned, halves[0], halves[1]))
            a_far.insert(0, jnp.where(aligned, halves[1], halves[0]))
        tail = PIECES[TAIL][0]
        before = PIECES[LATE][0]
        end = PIECES[last][0]
        half = far_product(a_far, both(0), None, 0, None, end)
        c = None
        for j in range(1, LATE + 1):
            start = PIECES[j][0]
            if j == LATE - 2:
                b_late, c = lax.optimization_barrier((b_blk, c))
                for i in range(LATE, LATEST):
                    send(i, b_late)
            if j == LATE:
                b_late, c = lax.optimization_barrier((b_blk, c))
                for i in range(LATEST, count):
                    send(i, b_late)
            if j == 1:
                half = pass_on(j, half)
            else:
                c = pass_on(j, c)
            if j < TAIL:
                vmem = 44 if j == TAIL - 1 else 62
                c = whole_product(a_near + a_far, b_blk, b_pair, x_own[j], x_pair[j], c, start, vmem)
            else:
                near, near_start = (sums_before, before) if j == LATE else (sums, tail)
                c = far_product(a_far, both(j), near, start - near_start, c, start)
            if j == 2:
                a_last, c = lax.optimization_barrier((a_far[1], c))
                a_last = a_last[:, row_of[last] :]
                a_last, c = lax.optimization_barrier((a_last, c))
            if j == NEAR_AFTER:
                a_near[0], c = lax.optimization_barrier((a_near[0], c))
                sums = near_sums(a_near, b_blk, b_pair, None, tail, before - tail)
                sums_before = near_sums(a_near, b_blk, b_pair, None, before, end - before)
                half = near_sums(a_near, b_blk, b_pair, half, end, b_blk.shape[1] - end)

        for j in range(LATE + 1, last):
            c = pass_on(j, c)
            half = far_product(a_far, both(j), half, 0, None, end)
            half, c = lax.optimization_barrier((half, c))
        half = pass_on(last, half)
        half = far_product(a_far, both(last)[:1], half, 0, None, end)
        c = last_product(a_last, x_pair[last], half, c, end)
        return c

    return jax.shard_map(
        local_product,
        mesh=mesh,
        in_specs=(P(("dp", "row"), "col"), P("row", "col")),
        out_specs=P(("dp", "row"), "col"),
        check_vma=False,
    )
```
